32 devices in a mesh: outer: 4 (over z), inner: 2 (over x), head: 4 (over y, core).
Axes of the slice: x: 2, y: 2, z: 4, core: 2. Of those that a mesh axis runs over, the one named last changes fastest.
Arguments:
- stored_query_rows: bfloat16 [2048, 32, 128], P(('outer', 'inner'), 'head'), may hold values from -12 to 12
- stored_key_rows: bfloat16 [2048, 8, 128], P(('outer', 'inner'), 'head'), may hold values from -12 to 12
- stored_value_rows: bfloat16 [2048, 8, 128], P(('outer', 'inner'), 'head'), may hold values from -6 to 6
- span_order: int32 [16], replicated, may hold values from 0 to 15, each once
Outputs:
- attended: bfloat16 [2048, 32, 128], P(('outer', 'inner'), 'head')
The draws below stay inside these ranges and needn't reach their ends.
Inputs may be any that keep to these rules, and one draw needn't show every extreme that they name: `span_order`: a permutation of the sequence's 16 blocks of 128 tokens.
All inputs are finite; a program needn't handle non-finite values.
Results may differ from the reference program's by a relative error of at most 0.0075.
Values may be sent and summed in bfloat16 or wider, within the bound.
A program may use at most 128 MiB of HBM per device.

```python
import math
import jax
import jax.numpy as jnp
from jax import lax

QUERY_HEADS = 32
KEY_VALUE_HEADS = 8
HEAD_DIMENSION = 128
BLOCK_TOKENS = 128
STORED_BLOCKS = 16
SEQUENCE_TOKENS = 2048


def draw_stored_query_rows(key, part):
    value_matrix = jnp.clip(jax.random.normal(jax.random.fold_in(key, 11), (SEQUENCE_TOKENS, QUERY_HEADS, HEAD_DIMENSION), jnp.float32), -6.0, 6.0)
    return value_matrix.astype(jnp.bfloat16)


def draw_stored_key_rows(key, part):
    value_matrix = jnp.clip(jax.random.normal(jax.random.fold_in(key, 12), (SEQUENCE_TOKENS, KEY_VALUE_HEADS, HEAD_DIMENSION), jnp.float32), -6.0, 6.0)
    return value_matrix.astype(jnp.bfloat16)


def block_levels(key, dims, shards, low, largest):
    level = 1.0
    for position, shards_of in shards:
        draws = jax.random.uniform(jax.random.fold_in(jax.random.fold_in(key, 6), position), (shards_of,), jnp.float32, low / len(shards), largest / len(shards))
        level = level * jnp.repeat(jnp.exp(draws), dims[position] // shards_of).reshape((-1,) + (1,) * (len(dims) - 1 - position))
    return level


def bell_draw(stream_key, dims, width, reach, pieces=(), held_as=jnp.bfloat16):
    entries = jax.random.normal(stream_key, dims, jnp.float32) * width
    if len(pieces) > 0:
        entries = block_levels(stream_key, dims, pieces, -0.22, 0.18) * entries
    return jnp.clip(entries, min=-reach, max=reach).astype(held_as)


def setup_inputs(seed: int = 0) -> dict:
    key_of = jax.random.split(jax.random.key(seed), 5)
    stored_query_rows = draw_stored_query_rows(jax.random.fold_in(key_of[4], 71), 0)
    stored_key_rows = draw_stored_key_rows(jax.random.fold_in(key_of[4], 71), 0)
    stored_value_rows = bell_draw(key_of[2], (SEQUENCE_TOKENS, KEY_VALUE_HEADS, HEAD_DIMENSION), 1.0, 6.0, ((0, 8), (1, 4)))
    span_order = jax.random.permutation(key_of[3], STORED_BLOCKS).astype(jnp.int32)
    return {"stored_query_rows": stored_query_rows, "stored_key_rows": stored_key_rows, "stored_value_rows": stored_value_rows, "span_order": span_order}


def attend_block(carry, query_tile, key_tile, value_tile, allowed, score_scale):
    run_max, run_sum, run_acc = carry
    scores = jnp.einsum('ghqa,kga->ghqk', query_tile.astype(jnp.float32), key_tile.astype(jnp.float32)) * score_scale
    scores = jnp.where(allowed[None, None], scores, -1e+30)
    new_max = jnp.maximum(run_max, lax.optimization_barrier(jnp.max(scores, axis=-1)))
    weights = jnp.where(allowed[None, None], jnp.exp(scores - new_max[..., None]), 0.0)
    rescale = jnp.exp(run_max - new_max)
    new_sum = run_sum * rescale + lax.optimization_barrier(jnp.sum(weights, axis=-1))
    rounded = lax.optimization_barrier(weights.astype(jnp.bfloat16)).astype(jnp.float32)
    added = jnp.einsum('ghqk,kga->ghqa', rounded, value_tile.astype(jnp.float32))
    return (new_max, new_sum, run_acc * rescale[..., None] + added)

def reference(stored_query_rows, stored_key_rows, stored_value_rows, span_order):
    heads_per_group = QUERY_HEADS // KEY_VALUE_HEADS
    inverse_permutation = jnp.zeros((STORED_BLOCKS,), jnp.int32).at[span_order].set(jnp.arange(STORED_BLOCKS, dtype=jnp.int32))
    query_in_order = stored_query_rows.reshape(STORED_BLOCKS, BLOCK_TOKENS, KEY_VALUE_HEADS, heads_per_group, HEAD_DIMENSION)[inverse_permutation].transpose(0, 2, 3, 1, 4)
    key_in_order = stored_key_rows.reshape(STORED_BLOCKS, BLOCK_TOKENS, KEY_VALUE_HEADS, HEAD_DIMENSION)[inverse_permutation]
    value_in_order = stored_value_rows.reshape(STORED_BLOCKS, BLOCK_TOKENS, KEY_VALUE_HEADS, HEAD_DIMENSION)[inverse_permutation]
    score_scale = 1.0 / math.sqrt(HEAD_DIMENSION)
    offsets = jnp.arange(BLOCK_TOKENS, dtype=jnp.int32)

    def one_span(index):
        query_tile = query_in_order[index]

        def visit(block, carry):
            allowed = (block * BLOCK_TOKENS + offsets)[None, :] <= (index * BLOCK_TOKENS + offsets)[:, None]
            return attend_block(carry, query_tile, key_in_order[block], value_in_order[block], allowed, score_scale)
        initial_state = (jnp.full((KEY_VALUE_HEADS, heads_per_group, BLOCK_TOKENS), -1e+30, jnp.float32), jnp.zeros((KEY_VALUE_HEADS, heads_per_group, BLOCK_TOKENS), jnp.float32), jnp.zeros((KEY_VALUE_HEADS, heads_per_group, BLOCK_TOKENS, HEAD_DIMENSION), jnp.float32))
        run_max, run_sum, run_acc = lax.fori_loop(0, index + 1, visit, initial_state)
        return run_acc / run_sum[..., None]
    result = lax.map(one_span, jnp.arange(STORED_BLOCKS, dtype=jnp.int32))
    result = result[span_order]
    return result.transpose(0, 3, 1, 2, 4).reshape(SEQUENCE_TOKENS, QUERY_HEADS, HEAD_DIMENSION).astype(jnp.bfloat16)
```

```python
import functools
import math

import jax
import jax.numpy as jnp
from jax import lax
from jax.experimental import pallas as pl
from jax.experimental.pallas import tpu as pltpu
from jax.sharding import PartitionSpec as P

MESH = pl.DeviceIdType.MESH
MASKED = -1e30
TILE = 256
CHUNKS = 2


def kernel(
    n_outer,
    n_inner,
    heads,
    span_ref,
    q_ref,
    kv_ref,
    o_ref,
    wide_ref,
    held,
    top_ref,
    sum_ref,
    acc_ref,
    send_up,
    send_down,
    send_across,
    recv_sem,
):
    rows, width = q_ref.shape
    kv_rows = kv_ref.shape[0]
    pair = kv_ref.shape[1] // 2
    span = kv_rows // 2
    chunk = kv_rows // CHUNKS
    tiles = rows // TILE
    factor = math.log2(math.e) / math.sqrt(width)
    outer = lax.axis_index("outer")
    inner = lax.axis_index("inner")

    barrier = pltpu.get_barrier_semaphore()

    @pl.when(outer > 0)
    def _():
        pl.semaphore_signal(barrier, inc=1, device_id={"outer": outer - 1}, device_id_type=MESH)

    @pl.when(outer < n_outer - 1)
    def _():
        pl.semaphore_signal(barrier, inc=1, device_id={"outer": outer + 1}, device_id_type=MESH)

    for step in range(1, n_inner):
        peer = lax.rem(inner + step, n_inner)
        pl.semaphore_signal(barrier, inc=1, device_id={"inner": peer}, device_id_type=MESH)

    ends = jnp.minimum(outer, 1) + jnp.minimum(n_outer - 1 - outer, 1)
    pl.semaphore_wait(barrier, n_inner - 1 + ends)

    def copy_of(source, src_outer, src_inner, part, send_sem, target):
        return pltpu.make_async_remote_copy(
            src_ref=source.at[pl.ds(part * chunk, chunk)],
            dst_ref=held.at[src_outer, src_inner, pl.ds(part * chunk, chunk)],
            send_sem=send_sem,
            recv_sem=recv_sem.at[src_outer, src_inner, part],
            device_id=target,
            device_id_type=MESH,
        )

    def up(source, src_outer, part):
        return copy_of(
            source, src_outer, inner, part, send_up.at[src_outer, part], {"outer": outer + 1}
        )

    def down(source, src_outer, part):
        return copy_of(
            source, src_outer, inner, part, send_down.at[src_outer, part], {"outer": outer - 1}
        )

    def across(source, src_outer, part, step):
        peer = lax.rem(inner + step, n_inner)
        return copy_of(
            source,
            src_outer,
            inner,
            part,
            send_across.at[src_outer, part, step - 1],
            {"inner": peer},
        )

    def pass_on(source, src_outer, part, act):
        @pl.when(jnp.logical_and(src_outer <= outer, outer < n_outer - 1))
        def _():
            act(up(source, src_outer, part))

        @pl.when(jnp.logical_and(src_outer >= outer, outer > 0))
        def _():
            act(down(source, src_outer, part))

        for step in range(1, n_inner):
            act(across(source, src_outer, part, step))

    def arrived(src_outer, src_inner, part):
        place = held.at[src_outer, src_inner, pl.ds(part * chunk, chunk)]
        pltpu.make_async_remote_copy(
            src_ref=place,
            dst_ref=place,
            send_sem=recv_sem.at[src_outer, src_inner, part],
            recv_sem=recv_sem.at[src_outer, src_inner, part],
            device_id={"inner": lax.rem(inner + 1, n_inner)},
            device_id_type=MESH,
        ).wait_recv()

    for part in range(CHUNKS):
        pass_on(kv_ref, outer, part, lambda copy: copy.start())

    row_head = lax.rem(lax.broadcasted_iota(jnp.int32, (TILE, width), 0), heads)
    first_head = row_head < heads // 2
    keep_first = jnp.where(first_head, 1.0, 0.0).astype(q_ref.dtype)
    keep_second = jnp.where(first_head, 0.0, 1.0).astype(q_ref.dtype)
    here = (outer * n_inner + inner) * 2
    lane = lax.broadcasted_iota(jnp.int32, (TILE, kv_rows), 1)

    def attend(block, value):
        pv = jnp.dot(block.astype(jnp.bfloat16), value, preferred_element_type=jnp.float32)
        return jnp.where(first_head, pv[:, :width], pv[:, width:])

    def scores_of(wide, key):
        return lax.dot_general(
            wide, key, (((1,), (1,)), ((), ())), preferred_element_type=jnp.float32
        )

    def own_tile(index, carry):
        at = pl.ds(pl.multiple_of(index * TILE, TILE), TILE)
        query = q_ref[at, :]
        wide = jnp.concatenate([query * keep_first, query * keep_second], axis=1)
        wide_ref[at, :] = wide
        scores = scores_of(wide, kv_ref[:, :pair])
        q_block = index // (tiles // 2)
        q_anchor = span_ref[here + q_block]
        row = lax.broadcasted_iota(jnp.int32, (TILE, kv_rows), 0)
        q_offset = (row + (index - q_block * (tiles // 2)) * TILE) // heads
        anchor = jnp.where(lane < span, span_ref[here], span_ref[here + 1])
        key_pos = anchor * span + lax.rem(lane, span)
        allowed = key_pos <= q_anchor * span + q_offset
        scores = jnp.where(allowed, scores, MASKED)
        top = jnp.max(scores, axis=1, keepdims=True)
        weights = jnp.exp2((scores - top) * factor)
        top_ref[at, :] = jnp.broadcast_to(top, (TILE, width))
        sum_ref[at, :] = weights[:, :width] + weights[:, width:]
        acc_ref[at, :] = attend(weights, kv_ref[:, pair:])
        return carry

    lax.fori_loop(0, tiles, own_tile, 0)

    def visit(src_outer, src_inner):
        base = (src_outer * n_inner + src_inner) * 2
        anchors = [span_ref[base], span_ref[base + 1]]
        place = held.at[src_outer, src_inner]

        def tile(index, carry):
            at = pl.ds(pl.multiple_of(index * TILE, TILE), TILE)
            q_anchor = span_ref[here + index // (tiles // 2)]
            bias = [jnp.where(anchor < q_anchor, 0.0, MASKED) for anchor in anchors]
            scores = scores_of(wide_ref[at, :], place[:, :pair])
            left = scores[:, :width] + bias[0]
            right = scores[:, width:] + bias[1]
            old = top_ref[at, :]
            top = jnp.maximum(old, jnp.max(jnp.maximum(left, right), axis=1, keepdims=True))
            rescale = jnp.exp2((old - top) * factor)
            left = jnp.exp2((left - top) * factor)
            right = jnp.exp2((right - top) * factor)
            top_ref[at, :] = top
            sum_ref[at, :] = sum_ref[at, :] * rescale + (left + right)
            weights = jnp.concatenate([left, right], axis=1)
            acc_ref[at, :] = acc_ref[at, :] * rescale + attend(weights, place[:, pair:])
            return carry

        lax.fori_loop(0, tiles, tile, 0, unroll=2)

    below = jnp.minimum(outer, n_outer - 1 - outer)

    def nth(step):
        paired = step <= 2 * below
        distance = jnp.where(paired, (step + 1) // 2, step - below)
        upward = jnp.where(
            paired, lax.rem(step, 2) == 0, outer < n_outer - 1 - outer
        )
        return jnp.where(upward, outer + distance, outer - distance)

    def from_inner(src_outer):
        for step in range(1, n_inner):
            src_inner = lax.rem(inner + step, n_inner)
            for part in range(CHUNKS):
                arrived(src_outer, src_inner, part)
            visit(src_outer, src_inner)

    def line_step(step, carry):
        src_outer = nth(step)
        for part in range(CHUNKS):
            arrived(src_outer, inner, part)
            pass_on(held.at[src_outer, inner], src_outer, part, lambda copy: copy.start())
        from_inner(nth(step - 1))
        visit(src_outer, inner)
        return carry

    lax.fori_loop(1, n_outer, line_step, 0)
    from_inner(nth(n_outer - 1))

    def finish(index, carry):
        at = pl.ds(pl.multiple_of(index * TILE, TILE), TILE)
        total = jnp.sum(sum_ref[at, :], axis=1, keepdims=True)
        o_ref[at, :] = (acc_ref[at, :] / total).astype(o_ref.dtype)
        return carry

    lax.fori_loop(0, tiles, finish, 0)

    def settle(src_outer, carry):
        for part in range(CHUNKS):
            pass_on(kv_ref, src_outer, part, lambda copy: copy.wait_send())
        return carry

    lax.fori_loop(0, n_outer, settle, 0)


def solution(mesh):
    n_outer, n_inner = mesh.shape["outer"], mesh.shape["inner"]

    def body(query, key, value, span_order):
        kv_rows, groups, width = key.shape
        heads = query.shape[1]
        rows = query.shape[0] * heads
        kv = jnp.concatenate(
            [key.reshape(kv_rows, groups * width), value.reshape(kv_rows, groups * width)], axis=1
        )
        vmem = pl.BlockSpec(memory_space=pltpu.VMEM)
        out = pl.pallas_call(
            functools.partial(kernel, n_outer, n_inner, heads),
            out_shape=jax.ShapeDtypeStruct((rows, width), jnp.bfloat16),
            in_specs=[pl.BlockSpec(memory_space=pltpu.SMEM), vmem, vmem],
            out_specs=vmem,
            scratch_shapes=[
                pltpu.VMEM((rows, groups * width), jnp.bfloat16),
                pltpu.VMEM((n_outer, n_inner) + kv.shape, jnp.bfloat16),
                pltpu.VMEM((rows, width), jnp.float32),
                pltpu.VMEM((rows, width), jnp.float32),
                pltpu.VMEM((rows, width), jnp.float32),
                pltpu.SemaphoreType.DMA((n_outer, CHUNKS)),
                pltpu.SemaphoreType.DMA((n_outer, CHUNKS)),
                pltpu.SemaphoreType.DMA((n_outer, CHUNKS, max(n_inner - 1, 1))),
                pltpu.SemaphoreType.DMA((n_outer, n_inner, CHUNKS)),
            ],
            compiler_params=pltpu.CompilerParams(
                collective_id=0, has_side_effects=True, vmem_limit_bytes=48 * 1024 * 1024
            ),
        )(span_order, query.reshape(rows, width), kv)
        return out.reshape(query.shape)

    placed = P(("outer", "inner"), "head", None)
    return jax.shard_map(
        body,
        mesh=mesh,
        in_specs=(placed, placed, placed, P()),
        out_specs=placed,
        check_vma=False,
    )
```

```python
import functools
import math

import jax
import jax.numpy as jnp
from jax import lax
from jax.experimental import pallas as pl
from jax.experimental.pallas import tpu as pltpu
from jax.sharding import PartitionSpec as P

MESH = pl.DeviceIdType.MESH
MASKED = -1e30
TILE = 512
CHUNKS = 2


def kernel(
    n_outer,
    n_inner,
    heads,
    span_ref,
    q_ref,
    kv_ref,
    o_ref,
    wide_ref,
    held,
    top_ref,
    sum_ref,
    acc_ref,
    send_up,
    send_down,
    send_across,
    recv_sem,
):
    rows, width = q_ref.shape
    kv_rows = kv_ref.shape[0]
    pair = kv_ref.shape[1] // 2
    span = kv_rows // 2
    chunk = kv_rows // CHUNKS
    tiles = rows // TILE
    factor = math.log2(math.e) / math.sqrt(width)
    outer = lax.axis_index("outer")
    inner = lax.axis_index("inner")

    barrier = pltpu.get_barrier_semaphore()

    @pl.when(outer > 0)
    def _():
        pl.semaphore_signal(barrier, inc=1, device_id={"outer": outer - 1}, device_id_type=MESH)

    @pl.when(outer < n_outer - 1)
    def _():
        pl.semaphore_signal(barrier, inc=1, device_id={"outer": outer + 1}, device_id_type=MESH)

    for step in range(1, n_inner):
        peer = lax.rem(inner + step, n_inner)
        pl.semaphore_signal(barrier, inc=1, device_id={"inner": peer}, device_id_type=MESH)

    ends = jnp.minimum(outer, 1) + jnp.minimum(n_outer - 1 - outer, 1)
    pl.semaphore_wait(barrier, n_inner - 1 + ends)

    def copy_of(source, src_outer, src_inner, part, send_sem, target):
        return pltpu.make_async_remote_copy(
            src_ref=source.at[pl.ds(part * chunk, chunk)],
            dst_ref=held.at[src_outer, src_inner, pl.ds(part * chunk, chunk)],
            send_sem=send_sem,
            recv_sem=recv_sem.at[src_outer, src_inner, part],
            device_id=target,
            device_id_type=MESH,
        )

    def up(source, src_outer, part):
        return copy_of(
            source, src_outer, inner, part, send_up.at[src_outer, part], {"outer": outer + 1}
        )

    def down(source, src_outer, part):
        return copy_of(
            source, src_outer, inner, part, send_down.at[src_outer, part], {"outer": outer - 1}
        )

    def across(source, src_outer, part, step):
        peer = lax.rem(inner + step, n_inner)
        return copy_of(
            source,
            src_outer,
            inner,
            part,
            send_across.at[src_outer, part, step - 1],
            {"inner": peer},
        )

    def pass_on(source, src_outer, part, act):
        @pl.when(jnp.logical_and(src_outer <= outer, outer < n_outer - 1))
        def _():
            act(up(source, src_outer, part))

        @pl.when(jnp.logical_and(src_outer >= outer, outer > 0))
        def _():
            act(down(source, src_outer, part))

        for step in range(1, n_inner):
            act(across(source, src_outer, part, step))

    def arrived(src_outer, src_inner, part):
        place = held.at[src_outer, src_inner, pl.ds(part * chunk, chunk)]
        pltpu.make_async_remote_copy(
            src_ref=place,
            dst_ref=place,
            send_sem=recv_sem.at[src_outer, src_inner, part],
            recv_sem=recv_sem.at[src_outer, src_inner, part],
            device_id={"inner": lax.rem(inner + 1, n_inner)},
            device_id_type=MESH,
        ).wait_recv()

    for part in range(CHUNKS):
        pass_on(kv_ref, outer, part, lambda copy: copy.start())

    row_head = lax.rem(lax.broadcasted_iota(jnp.int32, (TILE, width), 0), heads)
    first_head = row_head < heads // 2
    keep_first = jnp.where(first_head, 1.0, 0.0).astype(q_ref.dtype)
    keep_second = jnp.where(first_head, 0.0, 1.0).astype(q_ref.dtype)
    here = (outer * n_inner + inner) * 2
    lane = lax.broadcasted_iota(jnp.int32, (TILE, kv_rows), 1)

    def attend(block, value):
        pv = jnp.dot(block.astype(jnp.bfloat16), value, preferred_element_type=jnp.float32)
        return jnp.where(first_head, pv[:, :width], pv[:, width:])

    def scores_of(wide, key):
        return lax.dot_general(
            wide, key, (((1,), (1,)), ((), ())), preferred_element_type=jnp.float32
        )

    def at(index):
        return pl.ds(index * TILE, TILE)

    def own_scores(index):
        query = q_ref[at(index), :]
        wide = jnp.concatenate([query * keep_first, query * keep_second], axis=1)
        wide_ref[at(index), :] = wide
        return scores_of(wide, kv_ref[:, :pair])

    def visit_own():
        row = lax.broadcasted_iota(jnp.int32, (TILE, kv_rows), 0)
        anchor = jnp.where(lane < span, span_ref[here], span_ref[here + 1])
        ahead = anchor * span + lax.rem(lane, span) - row // heads
        scores = own_scores(0)
        for index in range(tiles):
            following = own_scores(index + 1) if index + 1 < tiles else None
            q_block = index // (tiles // 2)
            q_offset = (index - q_block * (tiles // 2)) * TILE // heads
            allowed = ahead <= span_ref[here + q_block] * span + q_offset
            scores = jnp.where(allowed, scores, MASKED)
            top = jnp.max(scores, axis=1, keepdims=True)
            weights = jnp.exp2((scores - top) * factor)
            top_ref[at(index), :] = jnp.broadcast_to(top, (TILE, width))
            sum_ref[at(index), :] = weights[:, :width] + weights[:, width:]
            acc_ref[at(index), :] = attend(weights, kv_ref[:, pair:])
            scores = following

    visit_own()

    def visit(src_outer, src_inner):
        base = (src_outer * n_inner + src_inner) * 2
        anchors = [span_ref[base], span_ref[base + 1]]
        place = held.at[src_outer, src_inner]

        def settle_sum(index, rescale, added):
            acc_ref[at(index), :] = acc_ref[at(index), :] * rescale + added

        scores = scores_of(wide_ref[at(0), :], place[:, :pair])
        waiting = None
        for index in range(tiles):
            following = None
            if index + 1 < tiles:
                following = scores_of(wide_ref[at(index + 1), :], place[:, :pair])
            q_anchor = span_ref[here + index // (tiles // 2)]
            bias = [jnp.where(anchor < q_anchor, 0.0, MASKED) for anchor in anchors]
            left = scores[:, :width] + bias[0]
            right = scores[:, width:] + bias[1]
            old = top_ref[at(index), :]
            top = jnp.maximum(old, jnp.max(jnp.maximum(left, right), axis=1, keepdims=True))
            rescale = jnp.exp2((old - top) * factor)
            left = jnp.exp2((left - top) * factor)
            right = jnp.exp2((right - top) * factor)
            top_ref[at(index), :] = top
            sum_ref[at(index), :] = sum_ref[at(index), :] * rescale + (left + right)
            weights = jnp.concatenate([left, right], axis=1)
            added = attend(weights, place[:, pair:])
            if waiting is not None:
                settle_sum(*waiting)
            waiting = (index, rescale, added)
            scores = following
        settle_sum(*waiting)

    below = jnp.minimum(outer, n_outer - 1 - outer)

    def nth(step):
        paired = step <= 2 * below
        distance = jnp.where(paired, (step + 1) // 2, step - below)
        upward = jnp.where(
            paired, lax.rem(step, 2) == 0, outer < n_outer - 1 - outer
        )
        return jnp.where(upward, outer + distance, outer - distance)

    def from_inner(src_outer):
        for step in range(1, n_inner):
            src_inner = lax.rem(inner + step, n_inner)
            for part in range(CHUNKS):
                arrived(src_outer, src_inner, part)
            visit(src_outer, src_inner)

    def line_step(step, carry):
        src_outer = nth(step)
        for part in range(CHUNKS):
            arrived(src_outer, inner, part)
            pass_on(held.at[src_outer, inner], src_outer, part, lambda copy: copy.start())
        from_inner(nth(step - 1))
        visit(src_outer, inner)
        return carry

    lax.fori_loop(1, n_outer, line_step, 0)
    from_inner(nth(n_outer - 1))

    for index in range(tiles):
        total = jnp.sum(sum_ref[at(index), :], axis=1, keepdims=True)
        o_ref[at(index), :] = (acc_ref[at(index), :] / total).astype(o_ref.dtype)

    def settle(src_outer, carry):
        for part in range(CHUNKS):
            pass_on(kv_ref, src_outer, part, lambda copy: copy.wait_send())
        return carry

    lax.fori_loop(0, n_outer, settle, 0)


def solution(mesh):
    n_outer, n_inner = mesh.shape["outer"], mesh.shape["inner"]

    def body(query, key, value, span_order):
        kv_rows, groups, width = key.shape
        heads = query.shape[1]
        rows = query.shape[0] * heads
        kv = jnp.concatenate(
            [key.reshape(kv_rows, groups * width), value.reshape(kv_rows, groups * width)], axis=1
        )
        vmem = pl.BlockSpec(memory_space=pltpu.VMEM)
        out = pl.pallas_call(
            functools.partial(kernel, n_outer, n_inner, heads),
            out_shape=jax.ShapeDtypeStruct((rows, width), jnp.bfloat16),
            in_specs=[pl.BlockSpec(memory_space=pltpu.SMEM), vmem, vmem],
            out_specs=vmem,
            scratch_shapes=[
                pltpu.VMEM((rows, groups * width), jnp.bfloat16),
                pltpu.VMEM((n_outer, n_inner) + kv.shape, jnp.bfloat16),
                pltpu.VMEM((rows, width), jnp.float32),
                pltpu.VMEM((rows, width), jnp.float32),
                pltpu.VMEM((rows, width), jnp.float32),
                pltpu.SemaphoreType.DMA((n_outer, CHUNKS)),
                pltpu.SemaphoreType.DMA((n_outer, CHUNKS)),
                pltpu.SemaphoreType.DMA((n_outer, CHUNKS, max(n_inner - 1, 1))),
                pltpu.SemaphoreType.DMA((n_outer, n_inner, CHUNKS)),
            ],
            compiler_params=pltpu.CompilerParams(
                collective_id=0, has_side_effects=True, vmem_limit_bytes=48 * 1024 * 1024
            ),
        )(span_order, query.reshape(rows, width), kv)
        return out.reshape(query.shape)

    placed = P(("outer", "inner"), "head", None)
    return jax.shard_map(
        body,
        mesh=mesh,
        in_specs=(placed, placed, placed, P()),
        out_specs=placed,
        check_vma=False,
    )
```

```python
import functools
import math

import jax
import jax.numpy as jnp
from jax import lax
from jax.experimental import pallas as pl
from jax.experimental.pallas import tpu as pltpu
from jax.sharding import PartitionSpec as P

MESH = pl.DeviceIdType.MESH
MASKED = -1e30
TILE = 512
CHUNKS = 4


def kernel(
    n_outer,
    n_inner,
    heads,
    span_hbm,
    q_ref,
    kv_ref,
    o_ref,
    span_ref,
    span_sem,
    wide_ref,
    held,
    top_ref,
    sum_ref,
    acc_ref,
    send_up,
    send_down,
    send_across,
    send_buddy,
    recv_sem,
):
    rows, width = q_ref.shape
    kv_rows = kv_ref.shape[0]
    pair = kv_ref.shape[1] // 2
    span = kv_rows // 2
    chunk = kv_rows // CHUNKS
    tiles = rows // TILE
    factor = math.log2(math.e) / math.sqrt(width)
    outer = lax.axis_index("outer")
    inner = lax.axis_index("inner")
    use_buddy = n_outer % 2 == 0 and n_outer > 2
    buddy = outer + 1 - 2 * lax.rem(outer, 2) if use_buddy else n_outer

    spans = pltpu.make_async_copy(span_hbm, span_ref, span_sem)
    spans.start()

    barrier = pltpu.get_barrier_semaphore()

    @pl.when(outer > 0)
    def _():
        pl.semaphore_signal(barrier, inc=1, device_id={"outer": outer - 1}, device_id_type=MESH)

    @pl.when(outer < n_outer - 1)
    def _():
        pl.semaphore_signal(barrier, inc=1, device_id={"outer": outer + 1}, device_id_type=MESH)

    for step in range(1, n_inner):
        peer = lax.rem(inner + step, n_inner)
        pl.semaphore_signal(barrier, inc=1, device_id={"inner": peer}, device_id_type=MESH)

    ends = jnp.minimum(outer, 1) + jnp.minimum(n_outer - 1 - outer, 1)
    pl.semaphore_wait(barrier, n_inner - 1 + ends)

    def copy_of(source, src_outer, src_inner, part, send_sem, target):
        return pltpu.make_async_remote_copy(
            src_ref=source.at[pl.ds(part * chunk, chunk)],
            dst_ref=held.at[src_outer, src_inner, pl.ds(part * chunk, chunk)],
            send_sem=send_sem,
            recv_sem=recv_sem.at[src_outer, src_inner, part],
            device_id=target,
            device_id_type=MESH,
        )

    def up(source, src_outer, part):
        return copy_of(
            source, src_outer, inner, part, send_up.at[src_outer, part], {"outer": outer + 1}
        )

    def down(source, src_outer, part):
        return copy_of(
            source, src_outer, inner, part, send_down.at[src_outer, part], {"outer": outer - 1}
        )

    def across(source, src_outer, part, step):
        peer = lax.rem(inner + step, n_inner)
        return copy_of(
            source,
            src_outer,
            inner,
            part,
            send_across.at[src_outer, part, step - 1],
            {"inner": peer},
        )

    def pass_on(source, src_outer, part, act):
        @pl.when(jnp.logical_and(src_outer <= outer, outer < n_outer - 1))
        def _():
            act(up(source, src_outer, part))

        @pl.when(jnp.logical_and(src_outer >= outer, outer > 0))
        def _():
            act(down(source, src_outer, part))

        @pl.when(jnp.logical_or(src_outer != buddy, part < CHUNKS // 2))
        def _():
            for step in range(1, n_inner):
                act(across(source, src_outer, part, step))

    def to_buddy(act):
        def one(step, carry):
            src_inner = lax.rem(inner + step, n_inner)
            for part in range(CHUNKS // 2, CHUNKS):
                act(
                    copy_of(
                        held.at[outer, src_inner],
                        outer,
                        src_inner,
                        part,
                        send_buddy.at[step - 1, part],
                        {"outer": buddy},
                    )
                )
            return carry

        lax.fori_loop(1, n_inner, one, 0)

    def arrived(src_outer, src_inner, part):
        place = held.at[src_outer, src_inner, pl.ds(part * chunk, chunk)]
        pltpu.make_async_remote_copy(
            src_ref=place,
            dst_ref=place,
            send_sem=recv_sem.at[src_outer, src_inner, part],
            recv_sem=recv_sem.at[src_outer, src_inner, part],
            device_id={"inner": lax.rem(inner + 1, n_inner)},
            device_id_type=MESH,
        ).wait_recv()

    for part in range(CHUNKS):
        pass_on(kv_ref, outer, part, lambda copy: copy.start())

    spans.wait()

    row_head = lax.rem(lax.broadcasted_iota(jnp.int32, (TILE, width), 0), heads)
    first_head = row_head < heads // 2
    keep_first = jnp.where(first_head, 1.0, 0.0).astype(q_ref.dtype)
    keep_second = jnp.where(first_head, 0.0, 1.0).astype(q_ref.dtype)
    here = (outer * n_inner + inner) * 2
    lane = lax.broadcasted_iota(jnp.int32, (TILE, kv_rows), 1)

    def attend(block, value):
        pv = jnp.dot(block.astype(jnp.bfloat16), value, preferred_element_type=jnp.float32)
        return jnp.where(first_head, pv[:, :width], pv[:, width:])

    def scores_of(wide, key):
        return lax.dot_general(
            wide, key, (((1,), (1,)), ((), ())), preferred_element_type=jnp.float32
        )

    def at(index):
        return pl.ds(index * TILE, TILE)

    def own_scores(index):
        query = q_ref[at(index), :]
        wide = jnp.concatenate([query * keep_first, query * keep_second], axis=1)
        wide_ref[at(index), :] = wide
        return scores_of(wide, kv_ref[:, :pair])

    def visit_own():
        row = lax.broadcasted_iota(jnp.int32, (TILE, kv_rows), 0)
        anchor = jnp.where(lane < span, span_ref[here], span_ref[here + 1])
        ahead = anchor * span + lax.rem(lane, span) - row // heads
        scores = own_scores(0)
        for index in range(tiles):
            following = own_scores(index + 1) if index + 1 < tiles else None
            q_block = index // (tiles // 2)
            q_offset = (index - q_block * (tiles // 2)) * TILE // heads
            allowed = ahead <= span_ref[here + q_block] * span + q_offset
            scores = jnp.where(allowed, scores, MASKED)
            top = jnp.max(scores, axis=1, keepdims=True)
            weights = jnp.exp2((scores - top) * factor)
            top_ref[at(index), :] = jnp.broadcast_to(top, (TILE, width))
            sum_ref[at(index), :] = weights[:, :width] + weights[:, width:]
            acc_ref[at(index), :] = attend(weights, kv_ref[:, pair:])
            scores = following

    visit_own()

    def visit(src_outer, src_inner):
        base = (src_outer * n_inner + src_inner) * 2
        anchors = [span_ref[base], span_ref[base + 1]]
        place = held.at[src_outer, src_inner]

        def settle_sum(index, rescale, added):
            acc_ref[at(index), :] = acc_ref[at(index), :] * rescale + added

        scores = scores_of(wide_ref[at(0), :], place[:, :pair])
        waiting = None
        for index in range(tiles):
            following = None
            if index + 1 < tiles:
                following = scores_of(wide_ref[at(index + 1), :], place[:, :pair])
            q_anchor = span_ref[here + index // (tiles // 2)]
            bias = [jnp.where(anchor < q_anchor, 0.0, MASKED) for anchor in anchors]
            left = scores[:, :width] + bias[0]
            right = scores[:, width:] + bias[1]
            old = top_ref[at(index), :]
            top = jnp.maximum(old, jnp.max(jnp.maximum(left, right), axis=1, keepdims=True))
            rescale = jnp.exp2((old - top) * factor)
            left = jnp.exp2((left - top) * factor)
            right = jnp.exp2((right - top) * factor)
            top_ref[at(index), :] = top
            sum_ref[at(index), :] = sum_ref[at(index), :] * rescale + (left + right)
            weights = jnp.concatenate([left, right], axis=1)
            added = attend(weights, place[:, pair:])
            if waiting is not None:
                settle_sum(*waiting)
            waiting = (index, rescale, added)
            scores = following
        settle_sum(*waiting)

    below = jnp.minimum(outer, n_outer - 1 - outer)

    def nth(step):
        paired = step <= 2 * below
        distance = jnp.where(paired, (step + 1) // 2, step - below)
        upward = jnp.where(
            paired, lax.rem(step, 2) == 0, outer < n_outer - 1 - outer
        )
        return jnp.where(upward, outer + distance, outer - distance)

    def from_inner(src_outer):
        def one(step, carry):
            src_inner = lax.rem(inner + step, n_inner)
            for part in range(CHUNKS):
                arrived(src_outer, src_inner, part)
            visit(src_outer, src_inner)
            return carry

        lax.fori_loop(1, n_inner, one, 0)

    def take(src_outer, parts):
        for part in parts:
            arrived(src_outer, inner, part)
            pass_on(held.at[src_outer, inner], src_outer, part, lambda copy: copy.start())

    def line_step(step, carry):
        take(nth(step), range(CHUNKS // 2))

        @pl.when(step > 1)
        def _():
            visit(nth(step - 1), inner)

        take(nth(step), range(CHUNKS // 2, CHUNKS))

        @pl.when(jnp.logical_and(step > 1, nth(step - 2) != buddy))
        def _():
            from_inner(nth(step - 2))

        return carry

    lax.fori_loop(1, n_outer, line_step, 0)
    if use_buddy:
        to_buddy(lambda copy: copy.start())
    visit(nth(n_outer - 1), inner)

    def last_step(step, carry):
        src_outer = jnp.where(step == 0, nth(n_outer - 2), nth(n_outer - 1))
        if use_buddy:
            src_outer = jnp.where(step == 1, buddy, src_outer)
            wanted = jnp.logical_or(step == 1, src_outer != buddy)
        else:
            wanted = step != 1

        @pl.when(wanted)
        def _():
            from_inner(src_outer)

        return carry

    lax.fori_loop(0, 3, last_step, 0)

    for index in range(tiles):
        total = jnp.sum(sum_ref[at(index), :], axis=1, keepdims=True)
        o_ref[at(index), :] = (acc_ref[at(index), :] / total).astype(o_ref.dtype)

    def settle(src_outer, carry):
        for part in range(CHUNKS):
            pass_on(kv_ref, src_outer, part, lambda copy: copy.wait_send())
        return carry

    lax.fori_loop(0, n_outer, settle, 0)
    if use_buddy:
        to_buddy(lambda copy: copy.wait_send())


def solution(mesh):
    n_outer, n_inner = mesh.shape["outer"], mesh.shape["inner"]

    def body(query, key, value, span_order):
        kv_rows, groups, width = key.shape
        heads = query.shape[1]
        rows = query.shape[0] * heads
        kv = jnp.concatenate(
            [key.reshape(kv_rows, groups * width), value.reshape(kv_rows, groups * width)], axis=1
        )
        vmem = pl.BlockSpec(memory_space=pltpu.VMEM)
        out = pl.pallas_call(
            functools.partial(kernel, n_outer, n_inner, heads),
            out_shape=jax.ShapeDtypeStruct((rows, width), jnp.bfloat16),
            in_specs=[pl.BlockSpec(memory_space=pltpu.HBM), vmem, vmem],
            out_specs=vmem,
            scratch_shapes=[
                pltpu.SMEM(span_order.shape, jnp.int32),
                pltpu.SemaphoreType.DMA,
                pltpu.VMEM((rows, groups * width), jnp.bfloat16),
                pltpu.VMEM((n_outer, n_inner) + kv.shape, jnp.bfloat16),
                pltpu.VMEM((rows, width), jnp.float32),
                pltpu.VMEM((rows, width), jnp.float32),
                pltpu.VMEM((rows, width), jnp.float32),
                pltpu.SemaphoreType.DMA((n_outer, CHUNKS)),
                pltpu.SemaphoreType.DMA((n_outer, CHUNKS)),
                pltpu.SemaphoreType.DMA((n_outer, CHUNKS, max(n_inner - 1, 1))),
                pltpu.SemaphoreType.DMA((max(n_inner - 1, 1), CHUNKS)),
                pltpu.SemaphoreType.DMA((n_outer, n_inner, CHUNKS)),
            ],
            compiler_params=pltpu.CompilerParams(
                collective_id=0, has_side_effects=True, vmem_limit_bytes=48 * 1024 * 1024
            ),
        )(span_order, query.reshape(rows, width), kv)
        return out.reshape(query.shape)

    placed = P(("outer", "inner"), "head", None)
    return jax.shard_map(
        body,
        mesh=mesh,
        in_specs=(placed, placed, placed, P()),
        out_specs=placed,
        check_vma=False,
    )
```
